32 devices in a mesh: dp: 4 (over z), vocab: 8 (over y, x, core).
Axes of the slice: x: 2, y: 2, z: 4, core: 2. Of those that a mesh axis runs over, the one named last changes fastest.
Arguments:
- hidden: bfloat16 [2560, 4096], P(('dp', 'vocab')), may hold values from -192 to 192, as said below
- out_weight: bfloat16 [4096, 20480], P('dp', 'vocab'), may hold values from -0.09375 to 0.09375
- labels: int32 [2560], P('dp'), may hold values from 0 to 20479
- text_mask: int32 [2560], P('dp'), may hold values from 0 to 1, as said below
Outputs:
- token_loss: float32 [2560], P('dp')
- mean_loss: float32 [], replicated
The draws below stay inside these ranges and needn't reach their ends.
Inputs may be any that keep to these rules, and one draw needn't show every extreme that they name: The hidden states are of moderate size in most rows, possibly larger in a few. `text_mask`: vision and text tokens come in runs of 16 aligned tokens.
All inputs are finite; a program needn't handle non-finite values.
Results may differ from the reference program's by a relative error of at most 0.0003.
Values may be sent and summed in bfloat16 or wider, within the bound.
No kernel may reach another device: no remote copies, remote signals or barrier semaphores. Data moves between devices by JAX's collectives and lax.ppermute only.
A program may use at most 128 MiB of HBM per device.

```python
import jax
import jax.numpy as jnp
from jax import lax

D = 4096
TOK_GROUP = 640
VOCAB = 20480
TOKENS = 2560
N_DP = 4


def draw_hidden(key, part):
    values = 3.0 * jax.random.truncated_normal(key, -4.0, 4.0, (TOKENS, D), jnp.float32)
    return values.astype(jnp.bfloat16)


def draw_text_mask(key, part):
    blocks = TOKENS // 16
    group_index = jnp.arange(blocks) * 16 // (TOKENS // N_DP)
    thresh = 25 + 50 * group_index // max(N_DP - 1, 1)
    rolled = jax.random.randint(key, (blocks,), 0, 100)
    is_text = (rolled < thresh).astype(jnp.int32)
    return jnp.repeat(is_text, 16)


def plant(result, rng, least, high):
    place = [jax.random.randint(jax.random.fold_in(rng, axis), (), 0, length) for axis, length in enumerate(result.shape)]
    widest = result.shape.index(max(result.shape))
    next_to = place[:widest] + [(place[widest] + 1) % result.shape[widest]] + place[widest + 1:]
    return result.at[tuple(place)].set(least).at[tuple(next_to)].set(high)


def steps_of(key, dims, split, least, top_value):
    def one(dim, parts):
        heights = jax.random.uniform(jax.random.fold_in(jax.random.fold_in(key, 6), dim), (parts,), jnp.float32, least / len(split), top_value / len(split))
        return jnp.repeat(jnp.exp(heights), dims[dim] // parts).reshape((-1,) + (1,) * (len(dims) - dim - 1))

    factor_of = one(*split[0])
    for cut in split[1:]:
        factor_of = factor_of * one(*cut)
    return factor_of


def centred(stream_key, dims, width, most, pieces=(), kind=jnp.bfloat16):
    drawn = width * jax.random.normal(stream_key, dims, jnp.float32)
    if pieces:
        drawn = drawn * steps_of(stream_key, dims, pieces, -0.22, 0.18)
    return jnp.clip(drawn, -most, most).astype(kind)


def setup_inputs(seed: int = 0) -> dict:
    key_of = jax.random.split(jax.random.key(seed), 5)
    hidden = draw_hidden(jax.random.fold_in(key_of[4], 71), 0)
    out_weight = centred(key_of[1], (D, VOCAB), D ** -0.5, 0.09375, ((0, 4), (1, 8)))
    labels = plant(jax.random.randint(key_of[2], (TOKENS,), 0, VOCAB), jax.random.fold_in(key_of[2], 1), 0, VOCAB - 1).astype(jnp.int32)
    text_mask = draw_text_mask(jax.random.fold_in(key_of[4], 71), 0)
    return {"hidden": hidden, "out_weight": out_weight, "labels": labels, "text_mask": text_mask}


def reference(hidden, out_weight, labels, text_mask):
    columns = jnp.arange(VOCAB, dtype=jnp.int32)

    def per_group(operand):
        states, targets = operand
        logits = jnp.dot(states, out_weight, preferred_element_type=jnp.float32)
        row_top = jnp.max(logits, axis=1)
        exp_total = jnp.sum(jnp.exp(logits - row_top[:, None]), axis=1)
        log_total = row_top + jnp.log(exp_total)
        picked = jnp.sum(jnp.where(columns[None, :] == targets[:, None], logits, jnp.float32(0.0)), axis=1)
        return log_total - picked

    losses = lax.map(per_group, (hidden.reshape(-1, TOK_GROUP, D), labels.reshape(-1, TOK_GROUP))).reshape(-1)
    weights_text = text_mask.astype(jnp.float32)
    token_loss = weights_text * losses
    tally = jnp.sum(weights_text)
    mean_loss = jnp.sum(token_loss) / jnp.maximum(tally, jnp.float32(1.0))
    return token_loss, mean_loss
```

```python
import functools

import jax
import jax.numpy as jnp
from jax import lax
from jax.experimental import pallas as pl
from jax.experimental.pallas import tpu as pltpu
from jax.sharding import PartitionSpec as P

DIRECT_PLANE = 8


def swap(a, axis, bit):
    n = lax.axis_size(axis)
    return lax.ppermute(a, axis, [(i, i ^ bit) for i in range(n)])


def main_kernel(n_z, early, late, chunk_counts, positions, *refs):
    flat = sum(chunk_counts)
    chunks, rest = refs[:flat], refs[flat:]
    weights, rest = rest[: len(early)], rest[len(early) :]
    acc_out, late_out, hid, acc, sem_in, sem_acc, sem_late = rest
    depth = weights[0].shape[0] if early[0][2] is None else None
    full = hid.shape[3]
    copies = []
    at = 0
    for g, count in enumerate(chunk_counts):
        group = []
        for c in range(count):
            ref = chunks[at]
            rows = ref.shape[0]
            row = pl.multiple_of(positions[n_z + c] * rows, rows) if count > 1 else 0
            for k in range(n_z):
                column = pl.multiple_of(positions[k] * full, full)
                copy = pltpu.make_async_copy(
                    ref.at[:, pl.ds(column, full)],
                    hid.at[g, k, pl.ds(row, rows), :],
                    sem_in.at[at, k],
                )
                copy.start()
                group.append(copy)
            at += 1
        copies.append(group)
    outs = []
    for g in range(len(chunk_counts)):
        for copy in copies[g]:
            copy.wait()
        for i, k in enumerate(late):
            out = pltpu.make_async_copy(hid.at[g, k], late_out.at[g, i], sem_late.at[g, i])
            out.start()
            outs.append(out)
        total = None
        for (k, start, size), w in zip(early, weights):
            term = jnp.dot(hid[g, k, :, start : start + size], w[...], preferred_element_type=jnp.float32)
            total = term if total is None else total + term
        acc[g] = total
        out = pltpu.make_async_copy(acc.at[g], acc_out.at[g], sem_acc.at[g])
        out.start()
        outs.append(out)
    for out in outs:
        out.wait()


def final_kernel(count, positions, acc, first, labels, *refs):
    hids, weights, out = refs[:count], refs[count : 2 * count], refs[2 * count]
    logits = acc[0]
    for h, w in zip(hids, weights):
        logits = logits + jnp.dot(h[0, 0], w[...], preferred_element_type=jnp.float32)
    rows, columns = logits.shape
    local = labels[0] - first[0]
    ids = lax.broadcasted_iota(jnp.int32, (rows, columns), 1)
    picked = jnp.sum(jnp.where(ids == local, logits, jnp.float32(0.0)), axis=1, keepdims=True)
    top = jnp.max(logits, axis=1, keepdims=True)
    total = jnp.sum(jnp.exp(logits - top), axis=1, keepdims=True)
    lse = top + jnp.log(total)
    lane = lax.broadcasted_iota(jnp.int32, (rows, 128), 1)
    both = jnp.where(lane == 0, lse, picked)
    out[0] = both.T[:8]


def shards(hidden, out_weight, labels, text_mask):
    n_z, n_v = lax.axis_size("dp"), lax.axis_size("vocab")
    z, v = lax.axis_index("dp"), lax.axis_index("vocab")
    rows, d_model = hidden.shape
    depth, width = out_weight.shape
    cols = width // n_z
    group = labels.shape[0]
    half = depth // 2

    held = {0: hidden}
    bit = n_z // 2
    while bit:
        for k in list(held):
            held[k | bit] = swap(held[k], "dp", bit)
        bit //= 2

    def piece(k, start, size):
        part = lax.dynamic_slice(out_weight, (0, (z ^ k) * cols), (depth, cols))
        part = lax.slice_in_dim(part, start, start + size, axis=0)
        return part if k == 0 else swap(part, "dp", k)

    chunks = []
    for k in range(n_z):
        if n_v <= DIRECT_PLANE:
            own = [held[k]] + [swap(held[k], "vocab", b) for b in range(2, n_v, 2)]
            both = [None] * n_v
            for i, part in enumerate(own):
                both[2 * i] = part
                both[2 * i + 1] = swap(part, "vocab", 1)
            chunks.append(both)
        else:
            chunks.append([lax.all_gather(held[k], "vocab", axis=0, tiled=True)])

    early = [(0, 0, depth), (1, 0, depth)] + [(k, 0, half) for k in range(2, n_z)]
    late = list(range(2, n_z))
    w_early = [piece(*e) for e in early]
    w_late = [piece(k, half, depth - half) for k in late]

    label_groups = jnp.stack([labels] + [swap(labels, "dp", k) for k in range(1, n_z)])
    mask_groups = jnp.stack([text_mask] + [swap(text_mask, "dp", k) for k in range(1, n_z)])
    which = z ^ jnp.arange(n_z, dtype=jnp.int32)
    hot = jnp.arange(n_z, dtype=jnp.int32)[:, None] == which[None, :]
    mask_all = jnp.sum(jnp.where(hot[:, :, None], mask_groups[None], 0), axis=1).astype(jnp.float32)
    tally = jnp.sum(mask_all)

    positions = jnp.concatenate([which, v ^ jnp.arange(n_v, dtype=jnp.int32)]).astype(jnp.int32)
    counts = [len(c) for c in chunks]
    flat = [a for c in chunks for a in c]
    any_space = pl.BlockSpec(memory_space=pl.ANY)
    in_vmem = pl.BlockSpec(memory_space=pltpu.VMEM)
    tokens = n_z * group
    acc, hid_late = pl.pallas_call(
        functools.partial(main_kernel, n_z, early, late, counts),
        out_shape=(
            jax.ShapeDtypeStruct((n_z, group, cols), jnp.float32),
            jax.ShapeDtypeStruct((n_z, len(late), group, depth), jnp.bfloat16),
        ),
        in_specs=[pl.BlockSpec(memory_space=pltpu.SMEM)] + [any_space] * len(flat) + [in_vmem] * len(early),
        out_specs=(any_space, any_space),
        scratch_shapes=[
            pltpu.VMEM((n_z, n_z, group, depth), jnp.bfloat16),
            pltpu.VMEM((n_z, group, cols), jnp.float32),
            pltpu.SemaphoreType.DMA((len(flat), n_z)),
            pltpu.SemaphoreType.DMA((n_z,)),
            pltpu.SemaphoreType.DMA((n_z, max(len(late), 1))),
        ],
        compiler_params=pltpu.CompilerParams(vmem_limit_bytes=60 << 20),
        cost_estimate=pl.CostEstimate(
            flops=2 * tokens * d_model * cols * 3 // 4, bytes_accessed=2 * tokens * d_model, transcendentals=0
        ),
        name="main",
    )(positions, *flat, *w_early)

    first = (v * width + z * cols).astype(jnp.int32).reshape(1)
    split = 2 if group % 256 == 0 else 1
    block = group // split
    stats = pl.pallas_call(
        functools.partial(final_kernel, len(late)),
        grid_spec=pltpu.PrefetchScalarGridSpec(
            num_scalar_prefetch=1,
            grid=(n_z, split),
            in_specs=[
                pl.BlockSpec((1, block, cols), lambda g, r, pos: (g, r, 0)),
                pl.BlockSpec(memory_space=pltpu.SMEM),
                pl.BlockSpec((1, block, 1), lambda g, r, pos: (g, r, 0)),
            ]
            + [
                pl.BlockSpec((1, 1, block, half), lambda g, r, pos, i=i: (g, i, r, 1)) for i in range(len(late))
            ]
            + [pl.BlockSpec((half, cols), lambda g, r, pos: (0, 0))] * len(late),
            out_specs=pl.BlockSpec((1, 8, block), lambda g, r, pos: (pos[g], 0, r)),
        ),
        out_shape=jax.ShapeDtypeStruct((n_z, 8, group), jnp.float32),
        compiler_params=pltpu.CompilerParams(vmem_limit_bytes=40 << 20),
        cost_estimate=pl.CostEstimate(
            flops=2 * tokens * d_model * cols // 4, bytes_accessed=8 * tokens * cols, transcendentals=tokens * cols
        ),
        name="final",
    )(positions, acc, first, label_groups[:, :, None], *([hid_late] * len(late)), *w_late)
    lse, picked = stats[:, 0], stats[:, 1]

    other_lse, other_picked = swap(lse, "vocab", 1), swap(picked, "vocab", 1)
    top = jnp.maximum(lse, other_lse)
    lse = top + jnp.log(jnp.exp(lse - top) + jnp.exp(other_lse - top))
    pair = jnp.stack([lse, picked + other_picked])
    pair = lax.dynamic_slice_in_dim(pair, (v % 2) * (group // 2), group // 2, axis=2)
    n_all = n_z * n_v
    sent = jnp.broadcast_to(pair[None], (n_all,) + pair.shape)
    got = lax.all_to_all(sent, ("dp", "vocab"), 0, 0, tiled=True)
    got = got.reshape(n_all // 2, 2, 2, n_z, group // 2)
    each, picks = got[:, :, 0], got[:, :, 1]
    top = jnp.max(each, axis=0)
    full_lse = top + jnp.log(jnp.sum(jnp.exp(each - top[None]), axis=0))
    loss = full_lse - jnp.sum(picks, axis=0)
    loss = jnp.moveaxis(loss, 0, 1).reshape(n_z, group) * mask_all
    mean_loss = jnp.sum(loss) / jnp.maximum(tally, jnp.float32(1.0))
    token_loss = lax.dynamic_index_in_dim(loss, z, 0, False)
    return token_loss, mean_loss


def solution(mesh):
    in_specs = (P(("dp", "vocab"), None), P("dp", "vocab"), P("dp"), P("dp"))
    out_specs = (P("dp"), P())
    return jax.shard_map(shards, mesh=mesh, in_specs=in_specs, out_specs=out_specs, check_vma=False)
```
